32 devices in a mesh: dp: 1 (over z), tp: 32 (over x, y, core).
Axes of the slice: x: 4, y: 4, z: 1, core: 2. Of those that a mesh axis runs over, the one named last changes fastest.
The devices are a block of a 4x4x8 slice.
Arguments:
- x: bfloat16 [7168, 5120], P(('dp', 'tp'))
- dy: bfloat16 [7168, 5120], P(('dp', 'tp'))
- gate: bfloat16 [7168, 12288], P('dp', 'tp')
- up: bfloat16 [7168, 12288], P('dp', 'tp')
- w_gate: bfloat16 [5120, 12288], P(None, 'tp')
- w_up: bfloat16 [5120, 12288], P(None, 'tp')
- w_down: bfloat16 [12288, 5120], P('tp')
Outputs:
- output 1: bfloat16 [7168, 5120], P(('dp', 'tp'))
- output 2: bfloat16 [5120, 12288], P('dp', 'tp')
- output 3: bfloat16 [5120, 12288], P('dp', 'tp')
- output 4: bfloat16 [12288, 5120], P(('dp', 'tp'))
All inputs are finite; a program needn't handle non-finite values.
Results may differ from the reference program's by a relative error of at most 0.012.
Values are sent between devices in bfloat16 or wider.
A program may use at most 768 MiB of HBM per device.

```python
import jax
import jax.numpy as jnp

ROWS = 7168
D = 5120
FF = 12288


def act(gate, up):
    return jax.nn.silu(gate) * up


def setup_inputs(seed: int = 0, part: int = 0) -> dict:
    kx, ky, ka, kb, kg, ku, kd = jax.random.split(jax.random.key(seed), 7)
    kx, ky, ka, kb = (jax.random.fold_in(k, part) for k in (kx, ky, ka, kb))
    drawn = {
        "x": jax.random.normal(kx, (ROWS, D), jnp.float32),
        "dy": jax.random.normal(ky, (ROWS, D), jnp.float32),
        "gate": jax.random.normal(ka, (ROWS, FF), jnp.float32),
        "up": jax.random.normal(kb, (ROWS, FF), jnp.float32),
        "w_gate": jax.random.normal(kg, (D, FF), jnp.float32) * D**-0.5,
        "w_up": jax.random.normal(ku, (D, FF), jnp.float32) * D**-0.5,
        "w_down": jax.random.normal(kd, (FF, D), jnp.float32) * FF**-0.5,
    }
    return {k: v.astype(jnp.bfloat16) for k, v in drawn.items()}


def reference(x, dy, gate, up, w_gate, w_up, w_down):
    hidden, back = jax.vjp(act, gate.astype(jnp.float32), up.astype(jnp.float32))
    d_hidden = jnp.dot(dy, w_down.T, preferred_element_type=jnp.float32)
    d_gate, d_up = (g.astype(jnp.bfloat16) for g in back(d_hidden))
    dx = jnp.dot(d_gate, w_gate.T, preferred_element_type=jnp.float32) + jnp.dot(d_up, w_up.T, preferred_element_type=jnp.float32)
    dw_gate = jnp.dot(x.T, d_gate, preferred_element_type=jnp.float32)
    dw_up = jnp.dot(x.T, d_up, preferred_element_type=jnp.float32)
    dw_down = jnp.dot(hidden.astype(jnp.bfloat16).T, dy, preferred_element_type=jnp.float32)
    return tuple(g.astype(jnp.bfloat16) for g in (dx, dw_gate, dw_up, dw_down))
```

```python
import functools
import math

import jax
import jax.numpy as jnp
from jax import lax
from jax.experimental import pallas as pl
from jax.experimental.pallas import tpu as pltpu
from jax.sharding import PartitionSpec as P

MESH = pl.DeviceIdType.MESH
BF, F32 = jnp.bfloat16, jnp.float32
CORES = 2
AG_DY, AG_X = 0, 16
WD, GA, UP, WG, WU, R_DWD, R_DW = 32, 33, 35, 37, 38, 39, 40
RS_PAIR, RS_Y, RS_T, N_SEM = 44, 52, 58, 60
FAR_OWN, FAR_OTHER, UP_OTHER, DN_OTHER, DN_OWN, UP_OWN = range(6)


def nt(a, b):
    return lax.dot_general(a, b, (((1,), (1,)), ((), ())), preferred_element_type=F32)


def kernel(
    side,
    x, dy, gate, up, wg, wu, wd,
    dx, dwg, dwu, dwd,
    dyh, xh, tr, gub, wdb, wgub, dgu, dgut, hdt, pair_s, pair_r, acc_s, acc_r, dwd_s, dwd_r, dw_s, dw_r,
    bounce, wdv, wv, lhs, ss, rs, loc,
):
    R, D = x.shape
    F = wd.shape[0]
    H = dyh.shape[0]
    half = H // 2
    me = lax.axis_index("tp")
    dp = lax.axis_index("dp")
    k = me % CORES
    cy = (me // CORES) % side
    cx = me // (CORES * side)

    def dev(a, b, c):
        return (dp, ((a + side) % side * side + (b + side) % side) * CORES + c)

    step = 1 - 2 * k
    fx, bx = (cx + step + side) % side, (cx - step + side) % side
    yp, ym = (cy + 1) % side, (cy + side - 1) % side
    yf = (cy + 2) % side
    ahead, behind = dev(fx, cy, k), dev(bx, cy, k)
    right, left = dev(cx, yp, k), dev(cx, ym, k)
    sibling = dev(cx, cy, 1 - k)
    own, other = cx // 2, 1 - cx // 2
    par = cx % 2

    def slot(h, b, c):
        return (h * side + b) * CORES + c

    def rows(s):
        return pl.ds(pl.multiple_of(s * R, R), R)

    def copy(i, src, dst, to):
        return pltpu.make_async_remote_copy(
            src_ref=src, dst_ref=dst, send_sem=ss.at[i], recv_sem=rs.at[i], device_id=to, device_id_type=MESH
        )

    sent = []

    def send(i, src, dst, to):
        c = copy(i, src, dst, to)
        c.start()
        sent.append((i, src, dst, to))

    def arrived(i, dst):
        copy(i, dst, dst, sibling).wait_recv()

    def local(src, dst, i):
        return pltpu.make_async_copy(src, dst, loc.at[i])

    barrier = pltpu.get_barrier_semaphore()
    for to in (ahead, behind, right, left, sibling):
        pl.semaphore_signal(barrier, inc=1, device_id=to, device_id_type=MESH)
    pl.semaphore_wait(barrier, 5)

    class Gather:
        def __init__(self, base, src, buf, t):
            self.b, self.src, self.buf, self.t = base, src, buf, t

        def at(self, s):
            return self.buf.at[rows(s)]

        def pass_on(self, i, s, to):
            send(self.b + i, self.at(s), self.at(s), to)

        def start(self):
            mine = self.at(slot(own, cy, k))
            send(self.b + 0, self.src, tr.at[self.t], ahead)
            send(self.b + 2, self.src, mine, right)
            send(self.b + 3, self.src, mine, left)
            send(self.b + 8, self.src, mine, sibling)

        def e1(self):
            arrived(self.b + 0, tr.at[self.t])
            s = self.at(slot(bx // 2, cy, k))
            send(self.b + 1, tr.at[self.t], s, ahead)

        def e2(self):
            s = slot(own, ym, k)
            arrived(self.b + 2, self.at(s))
            self.pass_on(6, s, right)
            self.pass_on(10, s, sibling)

        def e3(self):
            s = slot(own, yp, k)
            arrived(self.b + 3, self.at(s))
            self.pass_on(11, s, sibling)

        def e4(self):
            s = slot(other, cy, k)
            arrived(self.b + 1, self.at(s))
            self.pass_on(4, s, right)
            self.pass_on(5, s, left)
            self.pass_on(9, s, sibling)

        def e5(self):
            s = slot(other, ym, k)
            arrived(self.b + 4, self.at(s))
            self.pass_on(12, s, sibling)

        def e6(self):
            s = slot(other, yp, k)
            arrived(self.b + 5, self.at(s))
            self.pass_on(7, s, left)
            self.pass_on(13, s, sibling)

        def e7(self):
            s = slot(own, yf, k)
            arrived(self.b + 6, self.at(s))
            self.pass_on(14, s, sibling)

        def e8(self):
            s = slot(other, yf, k)
            arrived(self.b + 7, self.at(s))
            self.pass_on(15, s, sibling)

        def finish(self):
            c = 1 - k
            for i, (h, b) in enumerate(
                ((own, cy), (other, cy), (own, ym), (own, yp), (other, ym), (other, yp), (own, yf), (other, yf))
            ):
                arrived(self.b + 8 + i, self.at(slot(h, b, c)))

    gdy, gx = Gather(AG_DY, dy, dyh, 0), Gather(AG_X, x, xh, 1)
    gdy.start()
    ins = [local(dy, bounce.at[0], 0), local(x, bounce.at[1], 1), local(wd, wdv.at[pl.ds(0, F)], 2)]
    for c in ins:
        c.start()
    ins[0].wait()
    ins[1].wait()
    mine = rows(slot(own, cy, k))
    outs = [local(bounce.at[0], dyh.at[mine], 0), local(bounce.at[1], xh.at[mine], 1)]
    for c in outs:
        c.start()
    for c in outs:
        c.wait()
    ins[2].wait()

    gdy.e1()
    send(WD, wd, wdb, ahead)
    for i in range(2):
        theirs = pl.ds(pl.multiple_of((1 - par + 2 * i) * half, half), half)
        send(GA + i, gate.at[theirs], gub.at[0, pl.ds(i * half, half)], ahead)
        send(UP + i, up.at[theirs], gub.at[1, pl.ds(i * half, half)], ahead)
    gdy.e2()
    gdy.e3()
    gdy.e4()
    gdy.e5()
    gdy.e6()
    gx.start()
    gdy.e7()
    gdy.e8()
    gdy.finish()
    arrived(WD, wdb)
    c = local(wdb, wdv.at[pl.ds(F, F)], 2)
    c.start()
    for i in range(2):
        arrived(GA + i, gub.at[0, pl.ds(i * half, half)])
        arrived(UP + i, gub.at[1, pl.ds(i * half, half)])
    c.wait()

    TA = 256

    def act(dy_v, g0, u0, g1, u1, dgu_v, dgut_v, hdt_v):
        dh = nt(dy_v[...], wdv[...])
        for s, (g_v, u_v) in enumerate(((g0, u0), (g1, u1))):
            g, u = g_v[...].astype(F32), u_v[...].astype(F32)
            d = dh[:, s * F : (s + 1) * F]
            sig = jax.nn.sigmoid(g)
            silu = g * sig
            dg = d * u * (sig + silu * (1 - sig))
            du = d * silu
            for j, v in enumerate((dg, du)):
                at = slice((2 * s + j) * F, (2 * s + j + 1) * F)
                dgu_v[:, at] = v.astype(BF)
                dgut_v[at, :] = v.T.astype(BF)
            hdt_v[s * F : (s + 1) * F, :] = (silu * u).T.astype(BF)

    def act_half(h):
        at, theirs = pl.ds(h * half, half), pl.ds(pl.multiple_of((par + 2 * h) * half, half), half)
        rowmap = lambda i: (i, 0)
        colmap = lambda i: (0, i)
        pltpu.emit_pipeline(
            act,
            grid=(half // TA,),
            in_specs=[pl.BlockSpec((TA, D), rowmap)] + [pl.BlockSpec((TA, F), rowmap)] * 4,
            out_specs=[
                pl.BlockSpec((TA, 4 * F), rowmap),
                pl.BlockSpec((4 * F, TA), colmap),
                pl.BlockSpec((2 * F, TA), colmap),
            ],
        )(
            dyh.at[at], gate.at[theirs], up.at[theirs], gub.at[0, at], gub.at[1, at],
            dgu.at[at], dgut.at[:, at], hdt.at[:, at],
        )

    act_half(0)
    gx.e1()
    send(WG, wg, wgub.at[0], ahead)
    send(WU, wu, wgub.at[1], ahead)
    act_half(1)

    gx.e2()
    gx.e3()
    gx.e4()

    TN = 512

    def dwd_part(s, got, out):
        c = local(hdt.at[pl.ds(s * F, F)], lhs.at[pl.ds(0, F)], 2)
        c.start()
        c.wait()

        def body(dy_v, *refs):
            v = jnp.dot(lhs[:F, :], dy_v[...], preferred_element_type=F32)
            for r in refs[:-1]:
                v = v + r[...].astype(F32)
            refs[-1][...] = v.astype(BF)

        col = lambda i: (0, i)
        n = 0 if got is None else 1
        pltpu.emit_pipeline(
            body,
            grid=(D // TN,),
            in_specs=[pl.BlockSpec((H, TN), col)] + [pl.BlockSpec((F, TN), col)] * n,
            out_specs=[pl.BlockSpec((F, TN), col)],
        )(dyh, *([got] if n else []), out)

    dwd_part(1, None, dwd_s)
    send(R_DWD, dwd_s, dwd_r, behind)
    gx.e5()
    gx.e6()

    arrived(WG, wgub.at[0])
    arrived(WU, wgub.at[1])
    loads = [local(w, wv.at[:, pl.ds(i * F, F)], i) for i, w in enumerate((wg, wu, wgub.at[0], wgub.at[1]))]
    for c in loads:
        c.start()
    for c in loads:
        c.wait()
    gx.e7()

    TX = 512

    def dx_part(s, adds, out):
        def body(d_v, *refs):
            n = pl.program_id(0)
            v = nt(d_v[...], wv[pl.ds(pl.multiple_of(n * TX, TX), TX), :])
            for r in refs[:-1]:
                v = v + r[...].astype(F32)
            refs[-1][...] = v.astype(BF)

        col = lambda i: (0, i)
        pltpu.emit_pipeline(
            body,
            grid=(D // TX,),
            in_specs=[pl.BlockSpec((R, 4 * F), lambda i: (0, 0))] + [pl.BlockSpec((R, TX), col)] * len(adds),
            out_specs=[pl.BlockSpec((R, TX), col)],
        )(dgu.at[rows(s)], *adds, out)

    def for_sibling(j):
        h = (own + j % 2) % 2
        dx_part(slot(h, (cy + 2 + j // 2) % side, 1 - k), (), pair_s.at[j])
        copy(RS_PAIR + j, pair_s.at[j], pair_r.at[j], sibling).start()

    def from_sibling(t, i):
        j = 2 * i + t
        arrived(RS_PAIR + j, pair_r.at[j])
        return pair_r.at[j]

    def pass_sum(n, h, b, t, i, adds, to):
        dx_part(slot(h, b, k), (from_sibling(t, i), *adds), acc_s.at[n])
        send(RS_Y + n, acc_s.at[n], acc_r.at[n], to)

    def got(n):
        arrived(RS_Y + n, acc_r.at[n])
        return acc_r.at[n]

    lax.fori_loop(0, 2, lambda j, _: (for_sibling(j), 0)[1], 0)
    pass_sum(FAR_OWN, own, yf, 0, 0, (), right)
    pass_sum(FAR_OTHER, other, yf, 1, 0, (), left)
    gx.e8()
    gx.finish()

    cols = D // 2

    def dw_part(s, q, adds, outs):
        def body(x_v, *refs):
            v = jnp.dot(lhs[...], x_v[...], preferred_element_type=F32)
            for i in range(2):
                a = v[i * F : (i + 1) * F].T
                if adds:
                    a = a + refs[i][...].astype(F32)
                refs[len(adds) + i][...] = a.astype(BF)

        row = lambda i: (i, 0)
        pltpu.emit_pipeline(
            body,
            grid=(cols // TN,),
            in_specs=[pl.BlockSpec((H, TN), lambda i: (0, q * (cols // TN) + i))]
            + [pl.BlockSpec((TN, F), row)] * len(adds),
            out_specs=[pl.BlockSpec((TN, F), row)] * 2,
        )(xh, *adds, *outs)

    def load_lhs(s):
        c = local(dgut.at[pl.ds(s * 2 * F, 2 * F)], lhs, 2)
        c.start()
        c.wait()

    load_lhs(1)
    for q in range(2):
        dw_part(1, q, (), [dw_s.at[q, i] for i in range(2)])
        for i in range(2):
            send(R_DW + 2 * q + i, dw_s.at[q, i], dw_r.at[q, i], behind)
    lax.fori_loop(2, 8, lambda j, _: (for_sibling(j), 0)[1], 0)
    pass_sum(UP_OTHER, other, yp, 1, 3, (), right)
    pass_sum(DN_OTHER, other, ym, 1, 1, (got(FAR_OTHER),), left)
    pass_sum(DN_OWN, own, ym, 0, 1, (), left)
    pass_sum(UP_OWN, own, yp, 0, 3, (got(FAR_OWN),), right)
    arrived(R_DWD, dwd_r)
    dwd_part(0, dwd_r, dwd)
    dx_part(slot(other, cy, k), (from_sibling(1, 2), got(UP_OTHER), got(DN_OTHER)), acc_s.at[6])
    send(RS_T, acc_s.at[6], tr.at[2], ahead)
    load_lhs(0)
    for q in range(2):
        for i in range(2):
            arrived(R_DW + 2 * q + i, dw_r.at[q, i])
        dw_part(0, q, [dw_r.at[q, i] for i in range(2)], [w.at[pl.ds(q * cols, cols)] for w in (dwg, dwu)])
        if q == 0:
            arrived(RS_T, tr.at[2])
            send(RS_T + 1, tr.at[2], acc_r.at[6], ahead)
    arrived(RS_T + 1, acc_r.at[6])
    dx_part(slot(own, cy, k), (from_sibling(0, 2), got(UP_OWN), got(DN_OWN), acc_r.at[6]), dx)

    for a in sent:
        copy(*a).wait_send()
    for j in range(8):
        copy(RS_PAIR + j, pair_s.at[j], pair_r.at[j], sibling).wait_send()


def solution(mesh):
    side = math.isqrt(mesh.shape["tp"] // CORES)

    def body(x, dy, gate, up, w_gate, w_up, w_down):
        R, D = x.shape
        F = w_down.shape[0]
        H = gate.shape[0] // 2
        S = jax.ShapeDtypeStruct
        shapes = [
            S((R, D), BF), S((D, F), BF), S((D, F), BF), S((F, D), BF),
            S((H, D), BF), S((H, D), BF), S((3, R, D), BF), S((2, H, F), BF), S((F, D), BF), S((2, D, F), BF),
            S((H, 4 * F), BF), S((4 * F, H), BF), S((2 * F, H), BF),
            S((8, R, D), BF), S((8, R, D), BF), S((7, R, D), BF), S((7, R, D), BF),
            S((F, D), BF), S((F, D), BF), S((2, 2, D // 2, F), BF), S((2, 2, D // 2, F), BF),
        ]
        any_ = pl.BlockSpec(memory_space=pl.ANY)
        outs = pl.pallas_call(
            functools.partial(kernel, side),
            out_shape=shapes,
            in_specs=[any_] * 7,
            out_specs=[any_] * len(shapes),
            scratch_shapes=[
                pltpu.VMEM((2, R, D), BF),
                pltpu.VMEM((2 * F, D), BF),
                pltpu.VMEM((D, 4 * F), BF),
                pltpu.VMEM((2 * F, H), BF),
                pltpu.SemaphoreType.DMA((N_SEM,)),
                pltpu.SemaphoreType.DMA((N_SEM,)),
                pltpu.SemaphoreType.DMA((4,)),
            ],
            compiler_params=pltpu.CompilerParams(
                collective_id=0, has_side_effects=True, vmem_limit_bytes=62 * 1024 * 1024
            ),
        )(x, dy, gate, up, w_gate, w_up, w_down)
        return tuple(outs[:4])

    rows, cols, own = P(("dp", "tp"), None), P("dp", "tp"), P(None, "tp")
    return jax.shard_map(
        body,
        mesh=mesh,
        in_specs=(rows, rows, cols, cols, own, own, P("tp", None)),
        out_specs=(rows, cols, cols, P(("dp", "tp"), None)),
        check_vma=False,
    )
```

```python
import functools
import math

import jax
import jax.numpy as jnp
from jax import lax
from jax.experimental import pallas as pl
from jax.experimental.pallas import tpu as pltpu
from jax.sharding import PartitionSpec as P

MESH = pl.DeviceIdType.MESH
BF, F32 = jnp.bfloat16, jnp.float32
CORES = 2
AG_DY, AG_X = 0, 16
WD, GA, UP, WG, WU, R_DWD, R_DW = 32, 33, 35, 37, 38, 39, 40
RS_PAIR, RS_Y, RS_T, N_SEM = 44, 52, 58, 62
FAR_OWN, FAR_OTHER, UP_OTHER, DN_OTHER, DN_OWN, UP_OWN = range(6)


def nt(a, b):
    return lax.dot_general(a, b, (((1,), (1,)), ((), ())), preferred_element_type=F32)


def kernel(
    side,
    x, dy, gate, up, wg, wu, wd,
    dwg, dwu,
    dyh, xh, tr, own_gu, gub, wdb, wgub, dgu, dgut, hdt, pair_s, pair_r, acc_s, acc_r, part, dwd_s, dwd_r, dwd_f, dw_s, dw_r, dw_f,
    wv, wdt, lhs, ss, rs, loc,
):
    R, D = x.shape
    F = wd.shape[0]
    H = dyh.shape[0]
    half = H // 2
    me = lax.axis_index("tp")
    dp = lax.axis_index("dp")
    k = me % CORES
    cy = (me // CORES) % side
    cx = me // (CORES * side)

    def dev(a, b, c):
        return (dp, ((a + side) % side * side + (b + side) % side) * CORES + c)

    step = 1 - 2 * k
    fx, bx = (cx + step + side) % side, (cx - step + side) % side
    yp, ym = (cy + 1) % side, (cy + side - 1) % side
    yf = (cy + 2) % side
    ahead, behind = dev(fx, cy, k), dev(bx, cy, k)
    right, left = dev(cx, yp, k), dev(cx, ym, k)
    sibling = dev(cx, cy, 1 - k)
    own, other = cx // 2, 1 - cx // 2
    par = cx % 2

    def slot(h, b, c):
        return (h * side + b) * CORES + c

    def rows(s):
        return pl.ds(pl.multiple_of(s * R, R), R)

    def copy(i, src, dst, to):
        return pltpu.make_async_remote_copy(
            src_ref=src, dst_ref=dst, send_sem=ss.at[i], recv_sem=rs.at[i], device_id=to, device_id_type=MESH
        )

    def half_of(h):
        return pl.ds(pl.multiple_of(h * half, half), half)

    sent = []

    def send(i, src, dst, to):
        c = copy(i, src, dst, to)
        c.start()
        sent.append((i, src, dst, to))

    def arrived(i, dst):
        copy(i, dst, dst, sibling).wait_recv()

    def local(src, dst, i):
        return pltpu.make_async_copy(src, dst, loc.at[i])

    barrier = pltpu.get_barrier_semaphore()
    for to in (ahead, behind, right, left, sibling):
        pl.semaphore_signal(barrier, inc=1, device_id=to, device_id_type=MESH)
    pl.semaphore_wait(barrier, 5)

    class Gather:
        def __init__(self, base, src, buf, t):
            self.b, self.src, self.buf, self.t = base, src, buf, t

        def at(self, s):
            return self.buf.at[rows(s)]

        def pass_on(self, i, s, to):
            send(self.b + i, self.at(s), self.at(s), to)

        def start(self):
            mine = self.at(slot(own, cy, k))
            send(self.b + 0, self.src, tr.at[self.t], ahead)
            send(self.b + 2, self.src, mine, right)
            send(self.b + 3, self.src, mine, left)
            send(self.b + 8, self.src, mine, sibling)

        def e1(self):
            arrived(self.b + 0, tr.at[self.t])
            s = self.at(slot(bx // 2, cy, k))
            send(self.b + 1, tr.at[self.t], s, ahead)

        def e2(self):
            s = slot(own, ym, k)
            arrived(self.b + 2, self.at(s))
            self.pass_on(6, s, right)
            self.pass_on(10, s, sibling)

        def e3(self):
            s = slot(own, yp, k)
            arrived(self.b + 3, self.at(s))
            self.pass_on(11, s, sibling)

        def e4(self):
            s = slot(other, cy, k)
            arrived(self.b + 1, self.at(s))
            self.pass_on(4, s, right)
            self.pass_on(5, s, left)
            self.pass_on(9, s, sibling)

        def e5(self):
            s = slot(other, ym, k)
            arrived(self.b + 4, self.at(s))
            self.pass_on(12, s, sibling)

        def e6(self):
            s = slot(other, yp, k)
            arrived(self.b + 5, self.at(s))
            self.pass_on(7, s, left)
            self.pass_on(13, s, sibling)

        def e7(self):
            s = slot(own, yf, k)
            arrived(self.b + 6, self.at(s))
            self.pass_on(14, s, sibling)

        def e8(self):
            s = slot(other, yf, k)
            arrived(self.b + 7, self.at(s))
            self.pass_on(15, s, sibling)

        def finish_half(self, n):
            h = (own, other)[n]
            for i, b in zip(((8, 10, 11, 14), (9, 12, 13, 15))[n], (cy, ym, yp, yf)):
                arrived(self.b + i, self.at(slot(h, b, 1 - k)))

    gdy, gx = Gather(AG_DY, dy, dyh, 0), Gather(AG_X, x, xh, 1)
    gdy.start()

    rowmap = lambda i: (i, 0)
    colmap = lambda i: (0, i)
    TX = 1024

    def through(pairs, *shape):
        def go(buf):
            for leg in range(2):
                cs = [
                    local(*((buf.at[i], dst) if leg else (src, buf.at[i])), i) for i, (src, dst) in enumerate(pairs)
                ]
                for c in cs:
                    c.start()
                for c in cs:
                    c.wait()

        pl.run_scoped(go, pltpu.VMEM((len(pairs), *shape), BF))

    def turn_w(w, r):
        def body(t):
            at = pl.ds(pl.multiple_of(pl.program_id(0) * TX, TX), TX)
            wv[pl.ds(r * F, F), at] = t[...].T

        pltpu.emit_pipeline(body, grid=(D // TX,), in_specs=[pl.BlockSpec((TX, F), rowmap)])(w)

    def turn_wd(w, r):
        def body(t):
            at = pl.ds(pl.multiple_of(pl.program_id(0) * TX, TX), TX)
            wdt[at, pl.ds(r * F, F)] = t[...].T

        pltpu.emit_pipeline(body, grid=(D // TX,), in_specs=[pl.BlockSpec((F, TX), colmap)])(w)

    mine = rows(slot(own, cy, k))
    through([(dy, dyh.at[mine]), (x, xh.at[mine])], R, D)

    gdy.e1()
    send(WD, wd, wdb, ahead)
    for i in range(2):
        h = (fx // 2 + i) % 2
        theirs = pl.ds(pl.multiple_of((1 - par + 2 * h) * half, half), half)
        send(GA + i, gate.at[theirs], gub.at[0, half_of(h)], ahead)
        send(UP + i, up.at[theirs], gub.at[1, half_of(h)], ahead)
    turn_wd(wd, 0)
    gdy.e2()
    gdy.e3()
    gdy.e4()
    ours = [pl.ds(pl.multiple_of((par + 2 * i) * half, half), half) for i in range(2)]
    through([(a.at[ours[i]], own_gu.at[j, pl.ds(i * half, half)]) for j, a in enumerate((gate, up)) for i in range(2)], half, F)
    turn_w(wg, 0)
    turn_w(wu, 1)
    gdy.e6()
    gx.start()
    gdy.e7()
    arrived(WD, wdb)
    turn_wd(wdb, 1)
    TA = 256

    def act(dy_v, g0, u0, g1, u1, dgu_v, dgut_v, hdt_v):
        dh = jnp.dot(dy_v[...], wdt[...], preferred_element_type=F32)
        for s, (g_v, u_v) in enumerate(((g0, u0), (g1, u1))):
            g, u = g_v[...].astype(F32), u_v[...].astype(F32)
            d = dh[:, s * F : (s + 1) * F]
            sig = jax.nn.sigmoid(g)
            silu = g * sig
            dg = d * u * (sig + silu * (1 - sig))
            du = d * silu
            for j, v in enumerate((dg, du)):
                to = pl.ds((2 * s + j) * F, F)
                dgu_v[:, to] = v.astype(BF)
                dgut_v[to, :] = v.T.astype(BF)
            hdt_v[pl.ds(s * F, F), :] = (silu * u).T.astype(BF)

    def act_half(i, h):
        arrived(GA + i, gub.at[0, half_of(h)])
        arrived(UP + i, gub.at[1, half_of(h)])
        at = half_of(h)
        pltpu.emit_pipeline(
            act,
            grid=(half // TA,),
            in_specs=[pl.BlockSpec((TA, D), rowmap)] + [pl.BlockSpec((TA, F), rowmap)] * 4,
            out_specs=[
                pl.BlockSpec((TA, 4 * F), rowmap),
                pl.BlockSpec((4 * F, TA), colmap),
                pl.BlockSpec((2 * F, TA), colmap),
            ],
        )(
            dyh.at[at], own_gu.at[0, at], own_gu.at[1, at], gub.at[0, at], gub.at[1, at],
            dgu.at[at], dgut.at[:, at], hdt.at[:, at],
        )

    gdy.finish_half(0)
    act_half(0, own)
    gdy.e5()
    gdy.e8()
    gdy.finish_half(1)
    act_half(1, other)
    gx.e1()
    send(WG, wg, wgub.at[0], ahead)
    send(WU, wu, wgub.at[1], ahead)

    TN, WIDE = 512, 1024

    def load_lhs(src, r, n, halves=(0, 1)):
        cs = [
            local(src.at[pl.ds(r, n), pl.ds(pl.multiple_of(h * half, half), half)], lhs.at[i, pl.ds(0, n)], i)
            for i, h in enumerate(halves)
        ]
        for c in cs:
            c.start()
        for c in cs:
            c.wait()

    def dwd_part(out):
        def body(dy_v, o_v):
            v = jnp.dot(lhs[0, :F, :], dy_v[:half, :], preferred_element_type=F32)
            v += jnp.dot(lhs[1, :F, :], dy_v[half:, :], preferred_element_type=F32)
            o_v[...] = v.astype(o_v.dtype)

        pltpu.emit_pipeline(
            body,
            grid=(D // WIDE,),
            in_specs=[pl.BlockSpec((H, WIDE), colmap)],
            out_specs=[pl.BlockSpec((F, WIDE), colmap)],
        )(dyh, out)

    load_lhs(hdt, F, F)
    dwd_part(dwd_s)
    gx.e2()
    gx.e3()
    gx.e4()
    load_lhs(hdt, 0, F)
    dwd_part(dwd_f)
    arrived(WG, wgub.at[0])
    turn_w(wgub.at[0], 2)
    gx.e6()
    gx.e7()
    gx.finish_half(0)

    cols = D // 2

    def dw_half(i, h, q, n, tn, adds, outs):
        def body(x_v, *refs):
            v = jnp.dot(lhs[i], x_v[...], preferred_element_type=F32)
            for j in range(2):
                a = v[j * F : (j + 1) * F].T
                if adds:
                    a = a + refs[j][...]
                refs[len(adds) + j][...] = a.astype(refs[len(adds) + j].dtype)

        pltpu.emit_pipeline(
            body,
            grid=(n // tn,),
            in_specs=[pl.BlockSpec((half, tn), colmap)] + [pl.BlockSpec((tn, F), rowmap)] * len(adds),
            out_specs=[pl.BlockSpec((tn, F), rowmap)] * 2,
        )(xh.at[pl.ds(pl.multiple_of(h * half, half), half), pl.ds(q * n, n)], *adds, *outs)

    load_lhs(dgut, 2 * F, 2 * F, (own, other))
    dw_half(0, own, 0, D, WIDE, (), [dw_f.at[0], dw_f.at[1]])

    arrived(WU, wgub.at[1])
    send(R_DWD, dwd_s, dwd_r, behind)
    turn_w(wgub.at[1], 3)

    def dx_blocks(slots, adds, outs):
        m = len(slots)
        n_adds = sum(map(len, adds))

        def body(*refs):
            n = pl.program_id(0)
            d = jnp.concatenate([r[...] for r in refs[:m]], axis=0)
            at = pl.ds(pl.multiple_of(n * TX, TX), TX)
            v = jnp.dot(d, wv[:, at], preferred_element_type=F32)
            terms = iter(refs[m : m + n_adds])
            for j in range(m):
                a = v[j * R : (j + 1) * R]
                for _ in adds[j]:
                    a = a + next(terms)[...].astype(F32)
                o = refs[m + n_adds + j]
                o[...] = a.astype(o.dtype)

        tile = pl.BlockSpec((R, TX), colmap)
        pltpu.emit_pipeline(
            body,
            grid=(D // TX,),
            in_specs=[pl.BlockSpec((R, 4 * F), lambda i: (0, 0))] * m + [tile] * n_adds,
            out_specs=[tile] * m,
        )(*[dgu.at[rows(q)] for q in slots], *[a for b in adds for a in b], *outs)

    def dx_pairs(ys, c, adds, outs):
        dx_blocks([slot(h, b, c) for b in ys for h in (own, other)], adds, outs)

    def for_sibling(*ns):
        js = [2 * i + t for i in ns for t in range(2)]
        dx_pairs([(cy + 2 + i) % side for i in ns], 1 - k, [()] * len(js), [pair_s.at[j] for j in js])
        for j in js:
            send(RS_PAIR + j, pair_s.at[j], pair_r.at[j], sibling)

    def from_sibling(i):
        for j in (2 * i, 2 * i + 1):
            arrived(RS_PAIR + j, pair_r.at[j])
        return [(pair_r.at[2 * i],), (pair_r.at[2 * i + 1],)]

    def add(srcs, out):
        def body(*refs):
            v = refs[0][...]
            for r in refs[1:-1]:
                v = v + r[...].astype(F32)
            refs[-1][...] = v.astype(refs[-1].dtype)

        tile = pl.BlockSpec((32, D), rowmap)
        pltpu.emit_pipeline(body, grid=(R // 32,), in_specs=[tile] * len(srcs), out_specs=[tile])(*srcs, out)

    def got(n):
        arrived(RS_Y + n, acc_r.at[n])
        return acc_r.at[n]

    def pass_sum(n, to):
        send(RS_Y + n, acc_s.at[n], acc_r.at[n], to)

    for_sibling(0)
    gx.e5()
    gx.e8()
    dx_pairs([yf], k, from_sibling(0), [acc_s.at[FAR_OWN], acc_s.at[FAR_OTHER]])
    pass_sum(FAR_OWN, right)
    pass_sum(FAR_OTHER, left)
    gx.finish_half(1)

    def dw_rest(q):
        dw_half(1, other, q, cols, TN, [dw_f.at[i, pl.ds(q * cols, cols)] for i in range(2)], [dw_s.at[q, i] for i in range(2)])
        for i in range(2):
            send(R_DW + 2 * q + i, dw_s.at[q, i], dw_r.at[q, i], behind)

    dw_rest(0)
    for_sibling(1, 3)
    dw_rest(1)
    dx_pairs(
        [ym, yp], k, from_sibling(1) + from_sibling(3),
        [acc_s.at[DN_OWN], part.at[0], part.at[1], acc_s.at[UP_OTHER]],
    )
    pass_sum(UP_OTHER, right)
    add([part.at[0], got(FAR_OTHER)], acc_s.at[DN_OTHER])
    pass_sum(DN_OTHER, left)
    pass_sum(DN_OWN, left)
    add([part.at[1], got(FAR_OWN)], acc_s.at[UP_OWN])
    pass_sum(UP_OWN, right)
    for_sibling(2)

    def dw_own(q, lo, n):
        adds = [dw_r.at[q, i] for i in range(2)]
        if lo == 0:
            for i in range(2):
                arrived(R_DW + 2 * q + i, adds[i])

        def body(x_v, g_r, u_r, g_o, u_o):
            v = jnp.dot(lhs[0], x_v[:half, :], preferred_element_type=F32)
            v += jnp.dot(lhs[1], x_v[half:, :], preferred_element_type=F32)
            for j, (r, o) in enumerate(((g_r, g_o), (u_r, u_o))):
                o[...] = (v[j * F : (j + 1) * F].T + r[...].astype(F32)).astype(BF)

        at, part_ = pl.ds(q * cols + lo * TN, n * TN), pl.ds(lo * TN, n * TN)
        pltpu.emit_pipeline(
            body,
            grid=(n,),
            in_specs=[pl.BlockSpec((H, TN), colmap)] + [pl.BlockSpec((TN, F), rowmap)] * 2,
            out_specs=[pl.BlockSpec((TN, F), rowmap)] * 2,
        )(xh.at[:, at], *[a.at[part_] for a in adds], dwg.at[at], dwu.at[at])

    parts = [pl.ds(i * (R // 2), R // 2) for i in range(2)]

    def onward(i):
        arrived(RS_T + i, tr.at[2, parts[i]])
        send(RS_T + 2 + i, tr.at[2, parts[i]], acc_r.at[6, parts[i]], ahead)

    load_lhs(dgut, 0, 2 * F)
    tiles = cols // TN
    most = tiles - tiles // 2
    dw_own(0, 0, most)
    dx_pairs([cy], k, from_sibling(2), [part.at[2], part.at[3]])
    add([part.at[3], got(UP_OTHER), got(DN_OTHER)], acc_s.at[6])
    for i in range(2):
        send(RS_T + i, acc_s.at[6, parts[i]], tr.at[2, parts[i]], ahead)
    dw_own(0, most, tiles - most)
    onward(0)
    dw_own(1, 0, most)
    onward(1)
    dw_own(1, most, tiles - most)
    arrived(R_DWD, dwd_r)
    got(UP_OWN)
    got(DN_OWN)
    for i in range(2):
        arrived(RS_T + 2 + i, acc_r.at[6, parts[i]])

    for a in sent:
        copy(*a).wait_send()


def solution(mesh):
    side = math.isqrt(mesh.shape["tp"] // CORES)

    def body(x, dy, gate, up, w_gate, w_up, w_down):
        R, D = x.shape
        F = w_down.shape[0]
        H = gate.shape[0] // 2
        S = jax.ShapeDtypeStruct
        shapes = [
            S((D, F), BF), S((D, F), BF),
            S((H, D), BF), S((H, D), BF), S((3, R, D), BF), S((2, H, F), BF), S((2, H, F), BF), S((F, D), BF), S((2, D, F), BF),
            S((H, 4 * F), BF), S((4 * F, H), BF), S((2 * F, H), BF),
            S((8, R, D), BF), S((8, R, D), BF), S((7, R, D), BF), S((7, R, D), BF), S((4, R, D), F32),
            S((F, D), BF), S((F, D), BF), S((F, D), F32), S((2, 2, D // 2, F), BF), S((2, 2, D // 2, F), BF), S((2, D, F), F32),
        ]
        any_ = pl.BlockSpec(memory_space=pl.ANY)
        outs = pl.pallas_call(
            functools.partial(kernel, side),
            out_shape=shapes,
            in_specs=[any_] * 7,
            out_specs=[any_] * len(shapes),
            scratch_shapes=[
                pltpu.VMEM((4 * F, D), BF),
                pltpu.VMEM((D, 2 * F), BF),
                pltpu.VMEM((2, 2 * F, H // 2), BF),
                pltpu.SemaphoreType.DMA((N_SEM,)),
                pltpu.SemaphoreType.DMA((N_SEM,)),
                pltpu.SemaphoreType.DMA((8,)),
            ],
            compiler_params=pltpu.CompilerParams(
                collective_id=0, has_side_effects=True, vmem_limit_bytes=67_000_000
            ),
        )(x, dy, gate, up, w_gate, w_up, w_down)
        dwg, dwu = outs[:2]
        acc_r, part, _, dwd_r, dwd_f = outs[15:20]
        dx = part[2] + sum(acc_r[n].astype(F32) for n in (UP_OWN, DN_OWN, 6))
        dwd = dwd_f + dwd_r.astype(F32)
        return dx.astype(BF), dwg, dwu, dwd.astype(BF)

    rows, cols, own = P(("dp", "tp"), None), P("dp", "tp"), P(None, "tp")
    return jax.shard_map(
        body,
        mesh=mesh,
        in_specs=(rows, rows, cols, cols, own, own, P("tp", None)),
        out_specs=(rows, cols, cols, P(("dp", "tp"), None)),
        check_vma=False,
    )
```

```python
import functools
import math

import jax
import jax.numpy as jnp
from jax import lax
from jax.experimental import pallas as pl
from jax.experimental.pallas import tpu as pltpu
from jax.sharding import PartitionSpec as P

MESH = pl.DeviceIdType.MESH
BF, F32 = jnp.bfloat16, jnp.float32
CORES = 2
AG_DY, AG_X = 0, 16
WD, GA, UP, WG, WU, R_DWD, R_DW = 32, 33, 35, 37, 38, 39, 40
RS_PAIR, RS_Y, RS_T, N_SEM = 44, 52, 58, 62
FAR_OWN, FAR_OTHER, UP_OTHER, DN_OTHER, DN_OWN, UP_OWN = range(6)


def nt(a, b):
    return lax.dot_general(a, b, (((1,), (1,)), ((), ())), preferred_element_type=F32)


def kernel(
    side,
    x, dy, gate, up, wg, wu, wd,
    dwg, dwu,
    dyh, xh, tr, own_gu, gub, wdb, wgub, dgu, dgut, hdt, pair_s, pair_r, acc_s, acc_r, part, dwd_s, dwd_r, dwd_f, dw_s, dw_r, dw_f,
    wv, wdt, lhs, ss, rs, loc,
):
    R, D = x.shape
    F = wd.shape[0]
    H = dyh.shape[0]
    half = H // 2
    me = lax.axis_index("tp")
    dp = lax.axis_index("dp")
    k = me % CORES
    cy = (me // CORES) % side
    cx = me // (CORES * side)

    def dev(a, b, c):
        return (dp, ((a + side) % side * side + (b + side) % side) * CORES + c)

    step = 1 - 2 * k
    fx, bx = (cx + step + side) % side, (cx - step + side) % side
    yp, ym = (cy + 1) % side, (cy + side - 1) % side
    yf = (cy + 2) % side
    ahead, behind = dev(fx, cy, k), dev(bx, cy, k)
    right, left = dev(cx, yp, k), dev(cx, ym, k)
    sibling = dev(cx, cy, 1 - k)
    own, other = cx // 2, 1 - cx // 2
    par = cx % 2

    def slot(h, b, c):
        return (h * side + b) * CORES + c

    def rows(s):
        return pl.ds(pl.multiple_of(s * R, R), R)

    def copy(i, src, dst, to):
        return pltpu.make_async_remote_copy(
            src_ref=src, dst_ref=dst, send_sem=ss.at[i], recv_sem=rs.at[i], device_id=to, device_id_type=MESH
        )

    def half_of(h):
        return pl.ds(pl.multiple_of(h * half, half), half)

    sent = []

    def send(i, src, dst, to):
        c = copy(i, src, dst, to)
        c.start()
        sent.append((i, src, dst, to))

    def arrived(i, dst):
        copy(i, dst, dst, sibling).wait_recv()

    def local(src, dst, i):
        return pltpu.make_async_copy(src, dst, loc.at[i])

    barrier = pltpu.get_barrier_semaphore()
    for to in (ahead, behind, right, left, sibling):
        pl.semaphore_signal(barrier, inc=1, device_id=to, device_id_type=MESH)
    pl.semaphore_wait(barrier, 5)

    class Gather:
        def __init__(self, base, src, buf, t):
            self.b, self.src, self.buf, self.t = base, src, buf, t

        def at(self, s):
            return self.buf.at[rows(s)]

        def pass_on(self, i, s, to):
            send(self.b + i, self.at(s), self.at(s), to)

        def start(self):
            mine = self.at(slot(own, cy, k))
            send(self.b + 0, self.src, tr.at[self.t], ahead)
            send(self.b + 2, self.src, mine, right)
            send(self.b + 3, self.src, mine, left)
            send(self.b + 8, self.src, mine, sibling)

        def e1(self):
            arrived(self.b + 0, tr.at[self.t])
            s = self.at(slot(bx // 2, cy, k))
            send(self.b + 1, tr.at[self.t], s, ahead)

        def e2(self):
            s = slot(own, ym, k)
            arrived(self.b + 2, self.at(s))
            self.pass_on(6, s, right)
            self.pass_on(10, s, sibling)

        def e3(self):
            s = slot(own, yp, k)
            arrived(self.b + 3, self.at(s))
            self.pass_on(11, s, sibling)

        def e4(self):
            s = slot(other, cy, k)
            arrived(self.b + 1, self.at(s))
            self.pass_on(4, s, right)
            self.pass_on(5, s, left)
            self.pass_on(9, s, sibling)

        def e5(self):
            s = slot(other, ym, k)
            arrived(self.b + 4, self.at(s))
            self.pass_on(12, s, sibling)

        def e6(self):
            s = slot(other, yp, k)
            arrived(self.b + 5, self.at(s))
            self.pass_on(7, s, left)
            self.pass_on(13, s, sibling)

        def e7(self):
            s = slot(own, yf, k)
            arrived(self.b + 6, self.at(s))
            self.pass_on(14, s, sibling)

        def e8(self):
            s = slot(other, yf, k)
            arrived(self.b + 7, self.at(s))
            self.pass_on(15, s, sibling)

        def finish_half(self, n):
            h = (own, other)[n]
            for i, b in zip(((8, 10, 11, 14), (9, 12, 13, 15))[n], (cy, ym, yp, yf)):
                arrived(self.b + i, self.at(slot(h, b, 1 - k)))

    gdy, gx = Gather(AG_DY, dy, dyh, 0), Gather(AG_X, x, xh, 1)
    gdy.start()

    rowmap = lambda i: (i, 0)
    colmap = lambda i: (0, i)
    TX = 1024

    def through(pairs, *shape):
        def go(buf):
            for leg in range(2):
                cs = [
                    local(*((buf.at[i], dst) if leg else (src, buf.at[i])), i) for i, (src, dst) in enumerate(pairs)
                ]
                for c in cs:
                    c.start()
                for c in cs:
                    c.wait()

        pl.run_scoped(go, pltpu.VMEM((len(pairs), *shape), BF))

    def turn_w(w, r):
        def body(t):
            at = pl.ds(pl.multiple_of(pl.program_id(0) * TX, TX), TX)
            wv[pl.ds(r * F, F), at] = t[...].T

        pltpu.emit_pipeline(body, grid=(D // TX,), in_specs=[pl.BlockSpec((TX, F), rowmap)])(w)

    def turn_wd(w, r):
        def body(t):
            at = pl.ds(pl.multiple_of(pl.program_id(0) * TX, TX), TX)
            wdt[at, pl.ds(r * F, F)] = t[...].T

        pltpu.emit_pipeline(body, grid=(D // TX,), in_specs=[pl.BlockSpec((F, TX), colmap)])(w)

    mine = rows(slot(own, cy, k))
    through([(dy, dyh.at[mine]), (x, xh.at[mine])], R, D)

    gdy.e1()
    send(WD, wd, wdb, ahead)
    for i in range(2):
        h = (fx // 2 + i) % 2
        theirs = pl.ds(pl.multiple_of((1 - par + 2 * h) * half, half), half)
        send(GA + i, gate.at[theirs], gub.at[0, half_of(h)], ahead)
        send(UP + i, up.at[theirs], gub.at[1, half_of(h)], ahead)
    turn_wd(wd, 0)
    gdy.e2()
    gdy.e3()
    gdy.e4()
    ours = [pl.ds(pl.multiple_of((par + 2 * i) * half, half), half) for i in range(2)]
    through([(a.at[ours[i]], own_gu.at[j, pl.ds(i * half, half)]) for j, a in enumerate((gate, up)) for i in range(2)], half, F)
    turn_w(wg, 0)
    turn_w(wu, 1)
    gdy.e6()
    gx.start()
    gdy.e7()
    arrived(WD, wdb)
    turn_wd(wdb, 1)
    TA = 256

    def act(dy_v, g0, u0, g1, u1, dgu_v, dgut_v, hdt_v):
        dh = jnp.dot(dy_v[...], wdt[...], preferred_element_type=F32)
        for s, (g_v, u_v) in enumerate(((g0, u0), (g1, u1))):
            g, u = g_v[...].astype(F32), u_v[...].astype(F32)
            d = dh[:, s * F : (s + 1) * F]
            sig = jax.nn.sigmoid(g)
            silu = g * sig
            dg = d * u * (sig + silu * (1 - sig))
            du = d * silu
            for j, v in enumerate((dg, du)):
                to = pl.ds((2 * s + j) * F, F)
                dgu_v[:, to] = v.astype(BF)
                dgut_v[to, :] = v.T.astype(BF)
            hdt_v[pl.ds(s * F, F), :] = (silu * u).T.astype(BF)

    def act_half(i, h):
        arrived(GA + i, gub.at[0, half_of(h)])
        arrived(UP + i, gub.at[1, half_of(h)])
        at = half_of(h)
        pltpu.emit_pipeline(
            act,
            grid=(half // TA,),
            in_specs=[pl.BlockSpec((TA, D), rowmap)] + [pl.BlockSpec((TA, F), rowmap)] * 4,
            out_specs=[
                pl.BlockSpec((TA, 4 * F), rowmap),
                pl.BlockSpec((4 * F, TA), colmap),
                pl.BlockSpec((2 * F, TA), colmap),
            ],
        )(
            dyh.at[at], own_gu.at[0, at], own_gu.at[1, at], gub.at[0, at], gub.at[1, at],
            dgu.at[at], dgut.at[:, at], hdt.at[:, at],
        )

    gdy.finish_half(0)
    act_half(0, own)
    gdy.e5()
    gdy.e8()
    gdy.finish_half(1)
    act_half(1, other)
    gx.e1()
    send(WG, wg, wgub.at[0], ahead)
    send(WU, wu, wgub.at[1], ahead)

    TN, WIDE = 512, 1024

    def load_lhs(src, r, n, halves=(0, 1)):
        cs = [
            local(src.at[pl.ds(r, n), pl.ds(pl.multiple_of(h * half, half), half)], lhs.at[i, pl.ds(0, n)], i)
            for i, h in enumerate(halves)
        ]
        for c in cs:
            c.start()
        for c in cs:
            c.wait()

    def dwd_part(out):
        def body(dy_v, o_v):
            v = jnp.dot(lhs[0, :F, :], dy_v[:half, :], preferred_element_type=F32)
            v += jnp.dot(lhs[1, :F, :], dy_v[half:, :], preferred_element_type=F32)
            o_v[...] = v.astype(o_v.dtype)

        pltpu.emit_pipeline(
            body,
            grid=(D // WIDE,),
            in_specs=[pl.BlockSpec((H, WIDE), colmap)],
            out_specs=[pl.BlockSpec((F, WIDE), colmap)],
        )(dyh, out)

    load_lhs(hdt, F, F)
    dwd_part(dwd_s)
    gx.e2()
    gx.e3()
    gx.e4()
    load_lhs(hdt, 0, F)
    dwd_part(dwd_f)
    def dx_blocks(slots, adds, outs, depth=None):
        first, width = (0, 4 * F) if depth is None else (depth, 2 * F)
        m = len(slots)
        n_adds = sum(map(len, adds))

        def body(*refs):
            n = pl.program_id(0)
            d = jnp.concatenate([r[...] for r in refs[:m]], axis=0)
            at = pl.ds(pl.multiple_of(n * TX, TX), TX)
            v = jnp.dot(d, wv[pl.ds(first * width, width), at], preferred_element_type=F32)
            terms = iter(refs[m : m + n_adds])
            for j in range(m):
                a = v[j * R : (j + 1) * R]
                for _ in adds[j]:
                    a = a + next(terms)[...].astype(F32)
                o = refs[m + n_adds + j]
                o[...] = a.astype(o.dtype)

        tile = pl.BlockSpec((R, TX), colmap)
        pltpu.emit_pipeline(
            body,
            grid=(D // TX,),
            in_specs=[pl.BlockSpec((R, width), lambda i: (0, first))] * m + [tile] * n_adds,
            out_specs=[tile] * m,
        )(*[dgu.at[rows(q)] for q in slots], *[a for b in adds for a in b], *outs)

    def dx_pairs(ys, c, adds, outs, depth=None):
        dx_blocks([slot(h, b, c) for b in ys for h in (own, other)], adds, outs, depth)

    def for_sibling(*ns, adds=None, depth=None):
        js = [2 * i + t for i in ns for t in range(2)]
        dx_pairs([(cy + 2 + i) % side for i in ns], 1 - k, adds or [()] * len(js), [pair_s.at[j] for j in js], depth)
        for j in js:
            send(RS_PAIR + j, pair_s.at[j], pair_r.at[j], sibling)

    dx_pairs([yf], 1 - k, [(), ()], [part.at[0], part.at[1]], 0)
    dx_pairs([yf], k, [(), ()], [part.at[2], part.at[3]], 0)
    arrived(WG, wgub.at[0])
    turn_w(wgub.at[0], 2)
    gx.e6()
    gx.e7()
    gx.finish_half(0)

    cols = D // 2

    def dw_half(i, h, q, n, tn, adds, outs):
        def body(x_v, *refs):
            v = jnp.dot(lhs[i], x_v[...], preferred_element_type=F32)
            for j in range(2):
                a = v[j * F : (j + 1) * F].T
                if adds:
                    a = a + refs[j][...]
                refs[len(adds) + j][...] = a.astype(refs[len(adds) + j].dtype)

        pltpu.emit_pipeline(
            body,
            grid=(n // tn,),
            in_specs=[pl.BlockSpec((half, tn), colmap)] + [pl.BlockSpec((tn, F), rowmap)] * len(adds),
            out_specs=[pl.BlockSpec((tn, F), rowmap)] * 2,
        )(xh.at[pl.ds(pl.multiple_of(h * half, half), half), pl.ds(q * n, n)], *adds, *outs)

    load_lhs(dgut, 2 * F, 2 * F, (own, other))
    dw_half(0, own, 0, D, WIDE, (), [dw_f.at[0], dw_f.at[1]])

    arrived(WU, wgub.at[1])
    send(R_DWD, dwd_s, dwd_r, behind)
    turn_w(wgub.at[1], 3)

    def from_sibling(i):
        for j in (2 * i, 2 * i + 1):
            arrived(RS_PAIR + j, pair_r.at[j])
        return [(pair_r.at[2 * i],), (pair_r.at[2 * i + 1],)]

    def add(srcs, out):
        def body(*refs):
            v = refs[0][...]
            for r in refs[1:-1]:
                v = v + r[...].astype(F32)
            refs[-1][...] = v.astype(refs[-1].dtype)

        tile = pl.BlockSpec((32, D), rowmap)
        pltpu.emit_pipeline(body, grid=(R // 32,), in_specs=[tile] * len(srcs), out_specs=[tile])(*srcs, out)

    def got(n):
        arrived(RS_Y + n, acc_r.at[n])
        return acc_r.at[n]

    def pass_sum(n, to):
        send(RS_Y + n, acc_s.at[n], acc_r.at[n], to)

    for_sibling(0, adds=[(part.at[0],), (part.at[1],)], depth=1)
    gx.e5()
    gx.e8()
    dx_pairs(
        [yf], k, [(part.at[2 + t], *a) for t, a in enumerate(from_sibling(0))],
        [acc_s.at[FAR_OWN], acc_s.at[FAR_OTHER]], 1,
    )
    pass_sum(FAR_OWN, right)
    pass_sum(FAR_OTHER, left)
    gx.finish_half(1)

    def dw_rest(q):
        dw_half(1, other, q, cols, TN, [dw_f.at[i, pl.ds(q * cols, cols)] for i in range(2)], [dw_s.at[q, i] for i in range(2)])
        for i in range(2):
            send(R_DW + 2 * q + i, dw_s.at[q, i], dw_r.at[q, i], behind)

    dw_rest(0)
    for_sibling(1, 3)
    dw_rest(1)
    dx_pairs(
        [ym, yp], k, from_sibling(1) + from_sibling(3),
        [acc_s.at[DN_OWN], part.at[0], part.at[1], acc_s.at[UP_OTHER]],
    )
    pass_sum(UP_OTHER, right)
    add([part.at[0], got(FAR_OTHER)], acc_s.at[DN_OTHER])
    pass_sum(DN_OTHER, left)
    pass_sum(DN_OWN, left)
    add([part.at[1], got(FAR_OWN)], acc_s.at[UP_OWN])
    pass_sum(UP_OWN, right)
    def dw_own(q, lo, n):
        adds = [dw_r.at[q, i] for i in range(2)]
        if lo == 0:
            for i in range(2):
                arrived(R_DW + 2 * q + i, adds[i])

        def body(x_v, g_r, u_r, g_o, u_o):
            v = jnp.dot(lhs[0], x_v[:half, :], preferred_element_type=F32)
            v += jnp.dot(lhs[1], x_v[half:, :], preferred_element_type=F32)
            for j, (r, o) in enumerate(((g_r, g_o), (u_r, u_o))):
                o[...] = (v[j * F : (j + 1) * F].T + r[...].astype(F32)).astype(BF)

        at, part_ = pl.ds(q * cols + lo * TN, n * TN), pl.ds(lo * TN, n * TN)
        pltpu.emit_pipeline(
            body,
            grid=(n,),
            in_specs=[pl.BlockSpec((H, TN), colmap)] + [pl.BlockSpec((TN, F), rowmap)] * 2,
            out_specs=[pl.BlockSpec((TN, F), rowmap)] * 2,
        )(xh.at[:, at], *[a.at[part_] for a in adds], dwg.at[at], dwu.at[at])

    tiles = cols // TN
    few = tiles // 2
    for_sibling(2)
    load_lhs(dgut, 0, 2 * F)
    dw_own(0, 0, few)
    dx_pairs([cy], k, from_sibling(2), [part.at[2], part.at[3]])

    parts = [pl.ds(i * (R // 2), R // 2) for i in range(2)]

    def onward(i):
        arrived(RS_T + i, tr.at[2, parts[i]])
        send(RS_T + 2 + i, tr.at[2, parts[i]], acc_r.at[6, parts[i]], ahead)

    add([part.at[3], got(UP_OTHER), got(DN_OTHER)], acc_s.at[6])
    for i in range(2):
        send(RS_T + i, acc_s.at[6, parts[i]], tr.at[2, parts[i]], ahead)
    dw_own(0, few, tiles - few)
    onward(0)
    onward(1)
    dw_own(1, 0, tiles)
    arrived(R_DWD, dwd_r)
    got(UP_OWN)
    got(DN_OWN)
    for i in range(2):
        arrived(RS_T + 2 + i, acc_r.at[6, parts[i]])

    for a in sent:
        copy(*a).wait_send()


def solution(mesh):
    side = math.isqrt(mesh.shape["tp"] // CORES)

    def body(x, dy, gate, up, w_gate, w_up, w_down):
        R, D = x.shape
        F = w_down.shape[0]
        H = gate.shape[0] // 2
        S = jax.ShapeDtypeStruct
        shapes = [
            S((D, F), BF), S((D, F), BF),
            S((H, D), BF), S((H, D), BF), S((3, R, D), BF), S((2, H, F), BF), S((2, H, F), BF), S((F, D), BF), S((2, D, F), BF),
            S((H, 4 * F), BF), S((4 * F, H), BF), S((2 * F, H), BF),
            S((8, R, D), BF), S((8, R, D), BF), S((7, R, D), BF), S((7, R, D), BF), S((4, R, D), F32),
            S((F, D), BF), S((F, D), BF), S((F, D), F32), S((2, 2, D // 2, F), BF), S((2, 2, D // 2, F), BF), S((2, D, F), F32),
        ]
        any_ = pl.BlockSpec(memory_space=pl.ANY)
        outs = pl.pallas_call(
            functools.partial(kernel, side),
            out_shape=shapes,
            in_specs=[any_] * 7,
            out_specs=[any_] * len(shapes),
            scratch_shapes=[
                pltpu.VMEM((4 * F, D), BF),
                pltpu.VMEM((D, 2 * F), BF),
                pltpu.VMEM((2, 2 * F, H // 2), BF),
                pltpu.SemaphoreType.DMA((N_SEM,)),
                pltpu.SemaphoreType.DMA((N_SEM,)),
                pltpu.SemaphoreType.DMA((8,)),
            ],
            compiler_params=pltpu.CompilerParams(
                collective_id=0, has_side_effects=True, vmem_limit_bytes=67_000_000
            ),
        )(x, dy, gate, up, w_gate, w_up, w_down)
        dwg, dwu = outs[:2]
        acc_r, part, _, dwd_r, dwd_f = outs[15:20]
        dx = part[2] + sum(acc_r[n].astype(F32) for n in (UP_OWN, DN_OWN, 6))
        dwd = dwd_f + dwd_r.astype(F32)
        return dx.astype(BF), dwg, dwu, dwd.astype(BF)

    rows, cols, own = P(("dp", "tp"), None), P("dp", "tp"), P(None, "tp")
    return jax.shard_map(
        body,
        mesh=mesh,
        in_specs=(rows, rows, cols, cols, own, own, P("tp", None)),
        out_specs=(rows, cols, cols, P(("dp", "tp"), None)),
        check_vma=False,
    )
```
